32 devices in a mesh: rows: 8 (over y, x, core), feat: 4 (over z).
Axes of the slice: x: 2, y: 2, z: 4, core: 2. Of those that a mesh axis runs over, the one named last changes fastest.
Arguments:
- inputs: bfloat16 [16384, 512], P('rows'), may hold values from -6 to 6
- weight: bfloat16 [512, 8192], P(None, 'feat'), may hold values from -1.25 to 1.25
- phases: float32 [8192], P('feat'), may hold values from -3.140625 to 3.140625
- labels: int32 [16384], P('rows'), may hold values from 0 to 511
- prediction: bfloat16 [16384, 512], P('rows', 'feat'), may hold values from -4 to 4
- ridge_inverse: float32 [8192, 2048], P(('feat', 'rows')), may hold values from -2 to 2, as said below
- coefficients: float32 [8192, 512], P(('feat', 'rows')), may hold values from -6 to 6
Outputs:
- coefficients_out: float32 [8192, 512], P(('feat', 'rows'))
- residual_out: float32 [16384, 512], P('rows', 'feat')
The draws below stay inside these ranges and needn't reach their ends.
Inputs may be any that keep to these rules, and one draw needn't show every extreme that they name: `ridge_inverse`: each M_b is symmetric and positive definite.
All inputs are finite; a program needn't handle non-finite values.
Results may differ from the reference program's by a relative error of at most 0.003.
Values may be sent and summed in bfloat16 or wider, within the bound.
No kernel may reach another device: no remote copies, remote signals or barrier semaphores. Data moves between devices by JAX's collectives and lax.ppermute only.
A program may use at most 64 MiB of HBM per device.

```python
import math
import jax
import jax.numpy as jnp
from jax import lax

DIN = 512
FB = 2048
PANEL = 128
TICKS = 4
TOTAL_ROWS = 16384
FEATURES = 8192
CLASSES = 512
N_FEAT = 4


def draw_ridge_inverse(key, part):
    blocks_count = FEATURES // FB
    noise = jnp.clip(jax.random.normal(key, (blocks_count, FB, FB), jnp.float32), -5.0, 5.0)
    symmetric = noise + jnp.transpose(noise, (0, 2, 1))
    matrix = jnp.eye(FB, dtype=jnp.float32)[None] + 0.25 * symmetric / jnp.sqrt(jnp.float32(FB))
    return matrix.reshape(FEATURES, FB).astype(jnp.float32)


def with_ends(drawn, rng, smallest, top_value):
    index_at = [jax.random.randint(jax.random.fold_in(rng, axis), (), 0, length) for axis, length in enumerate(drawn.shape)]
    widest = drawn.shape.index(max(drawn.shape))
    neighbour = index_at[:widest] + [(index_at[widest] + 1) % drawn.shape[widest]] + index_at[widest + 1:]
    return drawn.at[tuple(index_at)].set(smallest).at[tuple(neighbour)].set(top_value)


def shard_levels(key, dims, pieces, low, high):
    def one(dim, shards_of):
        heights = jax.random.uniform(jax.random.fold_in(jax.random.fold_in(key, 6), dim), (shards_of,), jnp.float32, low / len(pieces), high / len(pieces))
        return jnp.repeat(jnp.exp(heights), dims[dim] // shards_of).reshape((-1,) + (1,) * (len(dims) - dim - 1))

    factor_of = one(*pieces[0])
    for cut in pieces[1:]:
        factor_of = factor_of * one(*cut)
    return factor_of


def normal_values(own_key, extent, spread, bound, pieces=(), held_as=jnp.bfloat16):
    values = spread * jax.random.normal(own_key, extent, jnp.float32)
    if pieces:
        values = values * shard_levels(own_key, extent, pieces, -0.22, 0.18)
    return jnp.clip(values, -bound, bound).astype(held_as)


def setup_inputs(seed: int = 0) -> dict:
    keys = jax.random.split(jax.random.key(seed), 8)
    return {
        "inputs": normal_values(keys[0], (TOTAL_ROWS, DIN), 1.0, 6.0, ((0, 8),)),
        "weight": normal_values(keys[1], (DIN, FEATURES), (DIN // 25) ** -0.5, 1.25, ((1, 4),)),
        "phases": jnp.clip(jax.random.uniform(keys[2], (FEATURES,), jnp.float32, -3.140625, 3.140625), -3.140625, 3.140625),
        "labels": with_ends(jax.random.randint(keys[3], (TOTAL_ROWS,), 0, CLASSES), jax.random.fold_in(keys[3], 1), 0, CLASSES - 1).astype(jnp.int32),
        "prediction": normal_values(keys[4], (TOTAL_ROWS, CLASSES), 0.5, 4.0, ((0, 8), (1, 4))),
        "ridge_inverse": draw_ridge_inverse(jax.random.fold_in(keys[7], 71), 0),
        "coefficients": normal_values(keys[6], (FEATURES, CLASSES), 1.0, 6.0, ((0, 32),), jnp.float32),
    }


ridge_weight = 0.5

def reference(inputs, weight, phases, labels, prediction, ridge_inverse, coefficients):
    scale = 1.0 / math.sqrt(TOTAL_ROWS)
    blocks = []
    for b in range(N_FEAT):
        linear = jnp.dot(inputs, weight[:, b * FB:(b + 1) * FB], preferred_element_type=jnp.float32) + phases[b * FB:(b + 1) * FB]
        blocks.append((jnp.cos(linear) * scale).astype(jnp.bfloat16))
    target = (labels[:, None] == jnp.arange(CLASSES, dtype=jnp.int32)[None, :]).astype(jnp.float32)
    residual = target - prediction.astype(jnp.float32)
    panels = [residual[:, q * PANEL:(q + 1) * PANEL] for q in range(N_FEAT)]
    coeffs = coefficients
    for tick in range(TICKS):
        for q in range(N_FEAT):
            b = (q + tick) % N_FEAT
            feature_block = blocks[b]
            correlation = jnp.dot(feature_block.T, panels[q].astype(jnp.bfloat16), preferred_element_type=jnp.float32)
            earlier = coeffs[b * FB:(b + 1) * FB, q * PANEL:(q + 1) * PANEL]
            right_side = correlation - ridge_weight * earlier
            change = jnp.dot(ridge_inverse[b * FB:(b + 1) * FB], right_side, precision=lax.Precision.HIGHEST, preferred_element_type=jnp.float32)
            coeffs = coeffs.at[b * FB:(b + 1) * FB, q * PANEL:(q + 1) * PANEL].set(earlier + change)
            panels[q] = panels[q] - jnp.dot(feature_block, change.astype(jnp.bfloat16), preferred_element_type=jnp.float32)
    ordered = [panels[(j - TICKS) % N_FEAT] for j in range(N_FEAT)]
    return (coeffs, jnp.concatenate(ordered, axis=1))
```

```python
import functools
import math

import jax
import jax.numpy as jnp
import numpy as np
from jax import lax
from jax.experimental import pallas as pl
from jax.experimental.pallas import tpu as pltpu
from jax.sharding import PartitionSpec as P

TICKS = 4


ridge_weight = 0.5
MIB = 1 << 20


def cosine_coefficients(degree, scale):
    nodes = (np.cos((np.arange(4096) + 0.5) * np.pi / 4096) + 1) / 8
    fit = np.polynomial.chebyshev.Chebyshev.fit(nodes, np.cos(2 * np.pi * np.sqrt(nodes)), degree, domain=[0, 0.25])
    plain = fit.convert(kind=np.polynomial.Polynomial, domain=[-1, 1], window=[-1, 1])
    return [float(c * scale) for c in plain.coef]


def strip_at(position, own, count):
    half = count // 2
    offset = jnp.where(position < half, 2 * position, 2 * (position - half) + 1)
    return own ^ offset


def features_body(own, inputs, weight, phases, stored, *, coefficients, chunk):
    per_turn = 1.0 / (2 * math.pi)
    magic = float(3 << 22)
    matrix = weight[...]
    offset = phases[...] * per_turn
    for start in range(0, inputs.shape[0], chunk):
        linear = jnp.dot(inputs[start:start + chunk, :], matrix, preferred_element_type=jnp.float32)
        turns = linear * per_turn + offset
        nearest = (turns + magic) - magic
        fraction = turns - nearest
        square = fraction * fraction
        value = jnp.full_like(square, coefficients[-1])
        for c in coefficients[-2::-1]:
            value = value * square + c
        stored[start:start + chunk, :] = value.astype(jnp.bfloat16)


def features(own, inputs, weight, phases, scale, count):
    rows, depth = inputs.shape
    width = weight.shape[1]
    strip = width // count
    body = functools.partial(features_body, coefficients=cosine_coefficients(6, scale), chunk=min(256, rows))
    return pl.pallas_call(
        body,
        grid_spec=pltpu.PrefetchScalarGridSpec(
            num_scalar_prefetch=1,
            grid=(count,),
            in_specs=[
                pl.BlockSpec((rows, depth), lambda j, own: (0, 0)),
                pl.BlockSpec((depth, strip), lambda j, own: (0, strip_at(j, own[0], count))),
                pl.BlockSpec((1, strip), lambda j, own: (0, strip_at(j, own[0], count))),
            ],
            out_specs=pl.BlockSpec((rows, strip), lambda j, own: (0, j)),
        ),
        out_shape=jax.ShapeDtypeStruct((rows, width), jnp.bfloat16),
        compiler_params=pltpu.CompilerParams(vmem_limit_bytes=20 * MIB),
        name="features",
    )(own, inputs, weight, phases.reshape(1, width))


def centred_body(own, matrix, result):
    size = matrix.shape[0]
    row = lax.broadcasted_iota(jnp.int32, matrix.shape, 0)
    col = lax.broadcasted_iota(jnp.int32, matrix.shape, 1)
    diagonal = (row == col) & (pl.program_id(0) == 0)
    result[...] = (matrix[...] - jnp.where(diagonal, 1.0, 0.0)).astype(jnp.bfloat16)


def centred(own, ridge_inverse, count):
    strip, width = ridge_inverse.shape
    return pl.pallas_call(
        centred_body,
        grid_spec=pltpu.PrefetchScalarGridSpec(
            num_scalar_prefetch=1,
            grid=(count,),
            in_specs=[pl.BlockSpec((strip, strip), lambda j, own: (0, strip_at(j, own[0], count)))],
            out_specs=pl.BlockSpec((strip, strip), lambda j, own: (0, j)),
        ),
        out_shape=jax.ShapeDtypeStruct((strip, width), jnp.bfloat16),
        compiler_params=pltpu.CompilerParams(vmem_limit_bytes=8 * MIB),
        name="centred",
    )(own, ridge_inverse)


def swapped(value, distance, count):
    return lax.ppermute(value, "rows", [(i, i ^ distance) for i in range(count)])


def passed_along(value, by):
    length = lax.axis_size("feat")
    return lax.ppermute(value, "feat", [(i, (i + by) % length) for i in range(length)])


def gathered(strip, count):
    near = jnp.concatenate([strip] + [swapped(strip, k, count) for k in range(2, count, 2)], axis=0)
    return jnp.concatenate([near, swapped(near, 1, count)], axis=0)


def scattered(kept, sent, count):
    size = kept.shape[0] // (count // 2)
    half = kept + swapped(sent.astype(jnp.bfloat16), 1, count).astype(jnp.float32)
    total = half[:size]
    for k in range(1, count // 2):
        piece = half[k * size:(k + 1) * size].astype(jnp.bfloat16)
        total = total + swapped(piece, 2 * k, count).astype(jnp.float32)
    return total


def on_device(inputs, weight, phases, labels, prediction, ridge_inverse, coefficients):
    count = lax.axis_size("rows")
    feat_count = lax.axis_size("feat")
    column = lax.axis_index("feat")
    own = lax.axis_index("rows").reshape(1).astype(jnp.int32)
    width = prediction.shape[1]
    scale = 1.0 / math.sqrt(inputs.shape[0] * count)
    shifted = labels[:, None] - column * width
    target = (shifted == jnp.arange(width, dtype=jnp.int32)[None, :]).astype(jnp.float32)
    residual = target - prediction.astype(jnp.float32)
    high = residual.astype(jnp.bfloat16)
    stored = features(own, inputs, weight, phases, scale, count)
    offset = centred(own, ridge_inverse, count)
    middle = weight.shape[1] // 2
    for tick in range(TICKS):
        start = ((column - tick) % feat_count) * width
        correlation = lax.dot_general(
            stored, high, (((0,), (0,)), ((), ())), preferred_element_type=jnp.float32
        )
        earlier = lax.dynamic_slice_in_dim(coefficients, start, width, 1)
        total = scattered(correlation[:middle], correlation[middle:], count)
        right_side = total - ridge_weight * earlier
        whole = gathered(right_side.astype(jnp.bfloat16), count)
        own_change = right_side + jnp.dot(offset, whole, preferred_element_type=jnp.float32)
        change = gathered(own_change.astype(jnp.bfloat16), count)
        coefficients = lax.dynamic_update_slice_in_dim(coefficients, earlier + own_change, start, 1)
        residual = residual - jnp.dot(stored, change, preferred_element_type=jnp.float32)
        rounded = lax.reduce_precision(residual, 8, 7)
        high = passed_along(rounded.astype(jnp.bfloat16), 1)
        low = passed_along((residual - rounded).astype(jnp.bfloat16), 1)
        residual = high.astype(jnp.float32) + low.astype(jnp.float32)
    return (coefficients, residual)


def solution(mesh):
    placed = (
        P("rows", None),
        P(None, "feat"),
        P("feat"),
        P("rows"),
        P("rows", "feat"),
        P(("feat", "rows"), None),
        P(("feat", "rows"), None),
    )
    return jax.shard_map(
        on_device,
        mesh=mesh,
        in_specs=placed,
        out_specs=(P(("feat", "rows"), None), P("rows", "feat")),
        check_vma=False,
    )
```
